8 devices in a mesh: dp: 8 (over z, y, x, core).
Axes of the slice: x: 2, y: 2, z: 1, core: 2. Of those that a mesh axis runs over, the one named last changes fastest.
Arguments:
- x_in: bfloat16 [32768, 896], P('dp')
- dy_mid: bfloat16 [32768, 4864], P('dp')
- x_mid: bfloat16 [32768, 4864], P('dp')
- dy_out: bfloat16 [32768, 896], P('dp')
- w_fc1: float32 [896, 4864], replicated
- w_fc2: float32 [4864, 896], replicated
- stat_left: float32 [40, 512, 512], P('dp')
- stat_right: float32 [40, 512, 512], P('dp')
- root_left: float32 [40, 512, 512], P('dp')
- root_right: float32 [40, 512, 512], P('dp')
- graft_sq: float32 [40, 512, 512], P('dp')
- momentum: float32 [40, 512, 512], P('dp')
Outputs:
- output 1: float32 [896, 4864], replicated
- output 2: float32 [4864, 896], replicated
- output 3: float32 [40, 512, 512], P('dp')
- output 4: float32 [40, 512, 512], P('dp')
- output 5: float32 [40, 512, 512], P('dp')
- output 6: float32 [40, 512, 512], P('dp')
All inputs are finite; a program needn't handle non-finite values.
Results may differ from the reference program's by a relative error of at most 0.001.
Values are sent between devices in bfloat16 or wider.
A program may use at most 1 GiB of HBM per device.

```python
import jax
import jax.numpy as jnp

D = 896
FF = 4864
BLOCK = 512
TOKENS = 4096
DEVICES = 8
STEP = 10

ROW_BLOCKS = (D + BLOCK - 1) // BLOCK
COL_BLOCKS = (FF + BLOCK - 1) // BLOCK
HALF_BLOCKS = ROW_BLOCKS * COL_BLOCKS
NUM_BLOCKS = 2 * HALF_BLOCKS
ROWS_ALL = DEVICES * TOKENS
STAT_DECAY = 0.999
MOM_DECAY = 0.9
GRAFT_EPS = 1e-8
LEARN_RATE = 0.01
WEIGHT_DECAY = 1e-4
BIAS_CORR = 1.0 - STAT_DECAY ** STEP


def spd_draw(key_pair, low_diag, high_diag):
    diag_key, factor_key = jax.random.split(key_pair)
    diag_vals = jax.random.uniform(diag_key, (NUM_BLOCKS, BLOCK), jnp.float32, low_diag, high_diag)
    factor = jax.random.normal(factor_key, (NUM_BLOCKS, BLOCK, 64), jnp.float32)
    low_rank = jnp.einsum('nik,njk->nij', factor, factor) / 128.0
    return low_rank + diag_vals[:, :, None] * jnp.eye(BLOCK, dtype=jnp.float32)


def setup_inputs(seed: int = 0) -> dict:
    key_list = jax.random.split(jax.random.key(seed), 12)
    grad_scale = TOKENS ** -0.5
    stat_scale = 0.01 * BLOCK / DEVICES
    x_in = jax.random.normal(key_list[0], (ROWS_ALL, D), jnp.float32).astype(jnp.bfloat16)
    dy_mid = (jax.random.normal(key_list[1], (ROWS_ALL, FF), jnp.float32) * grad_scale).astype(jnp.bfloat16)
    x_mid = jax.random.normal(key_list[2], (ROWS_ALL, FF), jnp.float32).astype(jnp.bfloat16)
    dy_out = (jax.random.normal(key_list[3], (ROWS_ALL, D), jnp.float32) * grad_scale).astype(jnp.bfloat16)
    w_fc1 = jax.random.normal(key_list[4], (D, FF), jnp.float32) * D ** -0.5
    w_fc2 = jax.random.normal(key_list[5], (FF, D), jnp.float32) * FF ** -0.5
    stat_left = stat_scale * spd_draw(key_list[6], 0.2, 1.0)
    stat_right = stat_scale * spd_draw(key_list[7], 0.2, 1.0)
    root_left = spd_draw(key_list[8], 0.2, 1.0)
    root_right = spd_draw(key_list[9], 0.2, 1.0)
    graft_sq = (BIAS_CORR / DEVICES) * jax.random.uniform(key_list[10], (NUM_BLOCKS, BLOCK, BLOCK), jnp.float32, 0.2, 2.0)
    momentum = jax.random.normal(key_list[11], (NUM_BLOCKS, BLOCK, BLOCK), jnp.float32)
    return {'x_in': x_in, 'dy_mid': dy_mid, 'x_mid': x_mid, 'dy_out': dy_out, 'w_fc1': w_fc1, 'w_fc2': w_fc2, 'stat_left': stat_left, 'stat_right': stat_right, 'root_left': root_left, 'root_right': root_right, 'graft_sq': graft_sq, 'momentum': momentum}


def to_blocks(matrix, row_blocks, col_blocks):
    padded = jnp.pad(matrix, ((0, row_blocks * BLOCK - matrix.shape[0]), (0, col_blocks * BLOCK - matrix.shape[1])))
    return padded.reshape(row_blocks, BLOCK, col_blocks, BLOCK).transpose(0, 2, 1, 3).reshape(row_blocks * col_blocks, BLOCK, BLOCK)


def from_blocks(blocks, row_blocks, col_blocks, n_rows, n_cols):
    full_mat = blocks.reshape(row_blocks, col_blocks, BLOCK, BLOCK).transpose(0, 2, 1, 3)
    return full_mat.reshape(row_blocks * BLOCK, col_blocks * BLOCK)[:n_rows, :n_cols]


def keep_mask(block_ids):
    is_first = block_ids < HALF_BLOCKS
    local_ids = block_ids % HALF_BLOCKS
    row_first = jnp.minimum(D - (local_ids // COL_BLOCKS) * BLOCK, BLOCK)
    col_first = jnp.minimum(FF - (local_ids % COL_BLOCKS) * BLOCK, BLOCK)
    row_second = jnp.minimum(FF - (local_ids // ROW_BLOCKS) * BLOCK, BLOCK)
    col_second = jnp.minimum(D - (local_ids % ROW_BLOCKS) * BLOCK, BLOCK)
    row_count = jnp.where(is_first, row_first, row_second)
    col_count = jnp.where(is_first, col_first, col_second)
    offsets = jnp.arange(BLOCK)
    return (offsets[None, :, None] < row_count[:, None, None]) & (offsets[None, None, :] < col_count[:, None, None])


def reference(x_in, dy_mid, x_mid, dy_out, w_fc1, w_fc2, stat_left, stat_right, root_left, root_right, graft_sq, momentum):
    grad_fc1 = jnp.dot(x_in.T, dy_mid, preferred_element_type=jnp.float32) / DEVICES
    grad_fc2 = jnp.dot(x_mid.T, dy_out, preferred_element_type=jnp.float32) / DEVICES
    grad_blk = jnp.concatenate([to_blocks(grad_fc1, ROW_BLOCKS, COL_BLOCKS), to_blocks(grad_fc2, COL_BLOCKS, ROW_BLOCKS)], axis=0)
    new_left = STAT_DECAY * stat_left + (1.0 - STAT_DECAY) * jnp.einsum('nik,njk->nij', grad_blk, grad_blk)
    new_right = STAT_DECAY * stat_right + (1.0 - STAT_DECAY) * jnp.einsum('nki,nkj->nij', grad_blk, grad_blk)
    precond = jnp.einsum('nij,njk->nik', jnp.einsum('nij,njk->nik', root_left, grad_blk), root_right)
    precond = jnp.where(keep_mask(jnp.arange(NUM_BLOCKS)), precond, 0.0)
    new_sq = STAT_DECAY * graft_sq + (1.0 - STAT_DECAY) * grad_blk * grad_blk
    graft_dir = grad_blk / (jnp.sqrt(new_sq / BIAS_CORR) + GRAFT_EPS)
    graft_norm = jnp.sqrt(jnp.sum(graft_dir * graft_dir, axis=(1, 2)))
    pre_norm = jnp.sqrt(jnp.sum(precond * precond, axis=(1, 2)))
    new_mom = MOM_DECAY * momentum + precond * (graft_norm / pre_norm)[:, None, None]
    direction = new_mom.astype(jnp.bfloat16).astype(jnp.float32)
    dir_fc1 = from_blocks(direction[:HALF_BLOCKS], ROW_BLOCKS, COL_BLOCKS, D, FF)
    dir_fc2 = from_blocks(direction[HALF_BLOCKS:], COL_BLOCKS, ROW_BLOCKS, FF, D)
    new_w1 = w_fc1 - LEARN_RATE * (dir_fc1 + WEIGHT_DECAY * w_fc1)
    new_w2 = w_fc2 - LEARN_RATE * (dir_fc2 + WEIGHT_DECAY * w_fc2)
    return (new_w1, new_w2, new_left, new_right, new_sq, new_mom)
```

```python
import functools

import jax
import jax.numpy as jnp
from jax import lax
from jax.experimental import pallas as pl
from jax.experimental.pallas import tpu as pltpu
from jax.sharding import PartitionSpec as P

STEP = 10
STAT_DECAY = 0.999
MOM_DECAY = 0.9
GRAFT_EPS = 1e-8
LEARN_RATE = 0.01
WEIGHT_DECAY = 1e-4
BIAS_CORR = 1.0 - STAT_DECAY ** STEP

MESH = pl.DeviceIdType.MESH
ANY = pl.BlockSpec(memory_space=pl.ANY)
BLK = 512
HALF = 256
STRIPS = 20
ROWS_OF = (512, 384)
F32 = jnp.float32
BF16 = jnp.bfloat16
VMEM_MAX = 66 * 1000 * 1000


def flip(dev, mask):
    for bit in (1, 2, 4):
        if mask & bit:
            dev = dev + bit - 2 * bit * ((dev // bit) % 2)
    return dev


def send(src, dst, send_sem, recv_sem, dev):
    return pltpu.make_async_remote_copy(src_ref=src, dst_ref=dst, send_sem=send_sem, recv_sem=recv_sem, device_id=(dev,), device_id_type=MESH)


def wait_bytes(ref, sem):
    pltpu.make_async_copy(ref, ref, sem).wait()


def greet(devs):
    barrier = pltpu.get_barrier_semaphore()
    for dev in devs:
        pl.semaphore_signal(barrier, inc=1, device_id=(dev,), device_id_type=MESH)
    pl.semaphore_wait(barrier, len(devs))


def strip_of(pos):
    return pos % 2, pos // 4 + 5 * ((pos // 2) % 2)


def owner_of(grad, strip, part):
    in_chip = jnp.where(grad == 0, strip, 2 * (strip % 5) + part)
    chip = jnp.where(grad == 0, part, 2 + strip // 5)
    return chip, in_chip // 5, in_chip % 5


def reduce_kernel(x_in, dy_mid, x_mid, dy_out, first, second, home, narrow, wide, out_buf, total, relay,
                  narrow_sem, wide_sem, pair_send, pair_recv, unit_sem, relay_sem, first_sem, second_sem, home_sem):
    me = lax.axis_index('dp')
    core = me % 2
    my_x, my_y = (me // 2) % 2, me // 4
    my_chip = me // 2
    partner = flip(me, 1)

    narrow_copies = [pltpu.make_async_copy(src, narrow.at[k], narrow_sem.at[k]) for k, src in enumerate((x_in, dy_out))]

    def load(job, pos, own):
        grad, strip = strip_of(pos)
        half = core if own else 1 - core
        off = pl.multiple_of(jnp.where(strip == 9, 9 * BLK, strip * BLK + half * HALF), HALF)
        slot = job % 3
        for k, src in enumerate((dy_mid, x_mid)):
            @pl.when(grad == k)
            def _():
                pltpu.make_async_copy(src.at[:, pl.ds(off, HALF)], wide.at[slot], wide_sem.at[slot]).start()

    def load_job(job):
        @pl.when((job % 2 == 1) & (job < 39))
        def _():
            load(job, (job + 1) // 2, False)
        @pl.when(job % 2 == 0)
        def _():
            load(job, job // 2 - 1, True)
        @pl.when(job == 39)
        def _():
            load(job, 19, True)

    narrow_copies[0].start()
    load(0, 0, False)
    load(1, 1, False)
    narrow_copies[1].start()
    greet([partner, flip(me, 2), flip(me, 3), flip(me, 4), flip(me, 5)])

    def piece(pos, slot, part):
        grad, _ = strip_of(pos)
        cols = pl.ds(part * 512, ROWS_OF[part])
        return lax.dot_general(narrow[grad, :, cols], wide[slot], (((0,), (0,)), ((), ())), preferred_element_type=F32)

    def give(pos, job):
        slot = job % 3
        wait_bytes(wide.at[slot], wide_sem.at[slot])
        sent = (pos < 18) | (pos - 18 != core)

        @pl.when(sent)
        def _():
            @pl.when(pos >= 2)
            def _():
                wait_bytes(out_buf.at[pos % 2], pair_send.at[pos % 2])
            for part in (0, 1):
                out_buf[pos % 2, pl.ds(part * 512, ROWS_OF[part]), :] = piece(pos, slot, part)
            send(out_buf.at[pos % 2], total.at[pos], pair_send.at[pos % 2], pair_recv.at[pos], partner).start()

    def unit(pos, part):
        grad, strip = strip_of(pos)
        chip, own_core, idx = owner_of(grad, strip, part)
        half = jnp.where(strip == 9, 0, core)
        dif_x, dif_y = my_x != chip % 2, my_y != chip // 2
        dif_a = jnp.where(core == 0, dif_x, dif_y)
        dif_b = jnp.where(core == 0, dif_y, dif_x)
        rows = pl.ds(0, ROWS_OF[part])
        src = total.at[pos, pl.ds(part * 512, ROWS_OF[part]), :]
        return dict(chip=chip, own_core=own_core, idx=idx, half=half, dif_a=dif_a, dif_b=dif_b, rows=rows, src=src,
                    sem=unit_sem.at[pos * 2 + part], dest=chip * 2 + own_core, slot=5 * own_core + idx)

    def keep(pos, job):
        slot = job % 3
        wait_bytes(wide.at[slot], wide_sem.at[slot])

        @pl.when((pos < 18) | (pos - 18 == core))
        def _():
            wait_bytes(total.at[pos], pair_recv.at[pos])
            for part in (0, 1):
                here = pl.ds(part * 512, ROWS_OF[part])
                total[pos, here, :] = total[pos, here, :] + piece(pos, slot, part)
                u = unit(pos, part)
                near, far = u['dif_a'] & ~u['dif_b'], u['dif_a'] & u['dif_b']
                mine = ~u['dif_a'] & ~u['dif_b']

                @pl.when(near)
                def _():
                    send(u['src'], first.at[u['idx'], u['half'], u['rows'], :], u['sem'], first_sem.at[u['idx'], u['half']], u['dest']).start()

                @pl.when(far & (core == 0))
                def _():
                    send(u['src'], relay.at[u['slot'], u['rows'], :], u['sem'], relay_sem.at[u['slot']], flip(me, 2)).start()

                @pl.when(far & (core == 1))
                def _():
                    send(u['src'], relay.at[u['slot'], u['rows'], :], u['sem'], relay_sem.at[u['slot']], flip(me, 4)).start()

                @pl.when(mine & (u['own_core'] == core))
                def _():
                    pltpu.make_async_copy(u['src'], home.at[u['idx'], u['half'], u['rows'], :], u['sem']).start()

                @pl.when(mine & (u['own_core'] != core))
                def _():
                    send(u['src'], home.at[u['idx'], u['half'], u['rows'], :], u['sem'], home_sem.at[u['idx']], partner).start()

    narrow_copies[0].wait()
    load(2, 0, True)
    give(0, 0)
    narrow_copies[1].wait()

    def step(pos, carry):
        job = 2 * pos - 1
        load_job(job + 2)
        give(pos, job)

        @pl.when(pos < 19)
        def _():
            load_job(job + 3)
        keep(pos - 1, job + 1)
        return carry

    lax.fori_loop(1, STRIPS, step, 0)
    keep(19, 39)

    for slot in (0, 1):
        wait_bytes(out_buf.at[slot], pair_send.at[slot])

    def hop(pos, carry):
        @pl.when((pos < 18) | (pos - 18 == core))
        def _():
            for part in (0, 1):
                u = unit(pos, part)

                @pl.when(~u['dif_a'] & u['dif_b'])
                def _():
                    here = pl.ds(part * 512, ROWS_OF[part])
                    wait_bytes(relay.at[u['slot'], u['rows'], :], relay_sem.at[u['slot']])
                    total[pos, here, :] = total[pos, here, :] + relay[u['slot'], u['rows'], :]
                    send(u['src'], second.at[u['idx'], u['half'], u['rows'], :], u['sem'], second_sem.at[u['idx'], u['half']], u['dest']).start()
        return carry
    lax.fori_loop(0, STRIPS, hop, 0)

    def drain(pos, carry):
        @pl.when((pos < 18) | (pos - 18 == core))
        def _():
            for part in (0, 1):
                u = unit(pos, part)
                wait_bytes(u['src'], u['sem'])
        return carry
    lax.fori_loop(0, STRIPS, drain, 0)

    def arrive(idx, carry):
        in_chip = 5 * core + idx
        on_first = my_chip < 2
        strip = jnp.where(on_first, in_chip, 5 * (my_chip - 2) + in_chip // 2)
        tall = jnp.where(on_first, my_chip, in_chip % 2)
        for half in (0, 1):
            source = jnp.where(strip == 9, jnp.where(on_first, 0, 1), half)
            for part in (0, 1):
                rows = pl.ds(0, ROWS_OF[part])

                @pl.when((tall == part) & ((strip < 9) | (half == 0)))
                def _():
                    wait_bytes(first.at[idx, half, rows, :], first_sem.at[idx, half])
                    wait_bytes(second.at[idx, half, rows, :], second_sem.at[idx, half])

                    @pl.when(source != core)
                    def _():
                        wait_bytes(home.at[idx, half, rows, :], home_sem.at[idx])
        return carry
    lax.fori_loop(0, 5, arrive, 0)


def reduce_grads(x_in, dy_mid, x_mid, dy_out):
    tokens, n_model = x_in.shape
    piece = jax.ShapeDtypeStruct((5, 2, BLK, HALF), F32)
    dma = pltpu.SemaphoreType.DMA
    return pl.pallas_call(
        reduce_kernel,
        out_shape=(piece, piece, piece),
        in_specs=[ANY] * 4,
        out_specs=(ANY, ANY, ANY),
        scratch_shapes=[
            pltpu.VMEM((2, tokens, n_model), BF16),
            pltpu.VMEM((3, tokens, HALF), BF16),
            pltpu.VMEM((2, n_model, HALF), F32),
            pltpu.VMEM((STRIPS, n_model, HALF), F32),
            pltpu.VMEM((10, BLK, HALF), F32),
            dma((2,)), dma((3,)), dma((2,)), dma((STRIPS,)), dma((2 * STRIPS,)), dma((10,)), dma((5, 2)), dma((5, 2)), dma((5,)),
        ],
        compiler_params=pltpu.CompilerParams(collective_id=0, has_side_effects=True, vmem_limit_bytes=VMEM_MAX),
        name='reduce_grads',
    )(x_in, dy_mid, x_mid, dy_out)


def dot3(a, b, dims):
    a_hi, b_hi = a.astype(BF16), b.astype(BF16)
    a_lo, b_lo = (a - a_hi.astype(F32)).astype(BF16), (b - b_hi.astype(F32)).astype(BF16)
    dot = functools.partial(lax.dot_general, dimension_numbers=(dims, ((), ())), preferred_element_type=F32)
    return dot(a_hi, b_hi) + (dot(a_hi, b_lo) + dot(a_lo, b_hi))


NN = ((1,), (0,))
NT = ((1,), (1,))
TN = ((0,), (0,))


def block_kernel(scale, first, second, home, left, right, root_left, root_right, sq, mom,
                 new_left, new_right, new_sq, new_mom, direction, grad_buf):
    me = lax.axis_index('dp')
    core, chip = me % 2, me // 2
    in_chip = 5 * core + pl.program_id(0)
    on_first = chip < 2
    strip = jnp.where(on_first, in_chip, 5 * (chip - 2) + in_chip // 2)
    tall = jnp.where(on_first, chip, in_chip % 2)
    n_rows = jnp.where(tall == 0, 512, 384)
    n_cols = jnp.where(strip == 9, 256, 512)
    row = lax.broadcasted_iota(jnp.int32, (BLK, BLK), 0)
    col = lax.broadcasted_iota(jnp.int32, (BLK, BLK), 1)
    grad_t = jnp.concatenate([(home[0, k] + first[0, k]) + second[0, k] for k in (0, 1)], axis=1) * scale
    grad_t = jnp.where((row < n_rows) & (col < n_cols), grad_t, 0.0)

    @pl.when(on_first)
    def _():
        grad_buf[...] = grad_t

    @pl.when(~on_first)
    def _():
        grad_buf[...] = grad_t.T
    grad = grad_buf[...]
    nat_rows = jnp.where(on_first, n_rows, n_cols)
    nat_cols = jnp.where(on_first, n_cols, n_rows)
    keep = (row < nat_rows) & (col < nat_cols)
    pre = dot3(dot3(root_left[0], grad, NN), root_right[0], NN)
    pre = jnp.where(keep, pre, 0.0)
    sq_now = STAT_DECAY * sq[0] + (1.0 - STAT_DECAY) * grad * grad
    new_sq[0] = sq_now
    graft = grad / (jnp.sqrt(sq_now / BIAS_CORR) + GRAFT_EPS)
    ratio = jnp.sqrt(jnp.sum(graft * graft, keepdims=True)) / jnp.sqrt(jnp.sum(pre * pre, keepdims=True))
    mom_now = MOM_DECAY * mom[0] + pre * ratio
    new_mom[0] = mom_now

    @pl.when(on_first)
    def _():
        direction[0] = mom_now.astype(BF16)

    @pl.when(~on_first)
    def _():
        direction[0] = mom_now.T.astype(BF16)
    new_left[0] = STAT_DECAY * left[0] + (1.0 - STAT_DECAY) * dot3(grad, grad, NT)
    new_right[0] = STAT_DECAY * right[0] + (1.0 - STAT_DECAY) * dot3(grad, grad, TN)


def block_update(n_dev, pieces, left, right, root_left, root_right, sq, mom):
    half_spec = pl.BlockSpec((1, 2, BLK, HALF), lambda i: (i, 0, 0, 0))
    tile_spec = pl.BlockSpec((1, BLK, BLK), lambda i: (i, 0, 0))
    tile = jax.ShapeDtypeStruct(left.shape, F32)
    return pl.pallas_call(
        functools.partial(block_kernel, 1.0 / n_dev),
        grid=(left.shape[0],),
        out_shape=(tile, tile, tile, tile, jax.ShapeDtypeStruct(left.shape, BF16)),
        in_specs=[half_spec] * 3 + [tile_spec] * 6,
        out_specs=(tile_spec,) * 5,
        scratch_shapes=[pltpu.VMEM((BLK, BLK), F32)],
        compiler_params=pltpu.CompilerParams(vmem_limit_bytes=VMEM_MAX),
        name='block_update',
    )(*pieces, left, right, root_left, root_right, sq, mom)


def gather_kernel(own, dirs, sends, recvs):
    me = lax.axis_index('dp')
    core = me % 2
    partner, x_dev, y_dev, far_dev = flip(me, 1), flip(me, 2), flip(me, 4), flip(me, 6)
    greet([partner, x_dev, y_dev])

    def tall_of(block):
        in_chip = block % 10
        return jnp.where(block < 20, block // 10, in_chip % 2)

    def move(block, lane, dev, src=None):
        for part in (0, 1):
            rows = pl.ds(0, ROWS_OF[part])

            @pl.when(tall_of(block) == part)
            def _():
                ref = dirs.at[block] if src is None else src
                send(ref.at[rows, :], dirs.at[block, rows, :], sends.at[block, lane], recvs.at[block], dev).start()

    def landed(block, sem):
        for part in (0, 1):
            @pl.when(tall_of(block) == part)
            def _():
                wait_bytes(dirs.at[block, pl.ds(0, ROWS_OF[part]), :], sem)

    def begin(i, carry):
        block = me * 5 + i
        pltpu.make_async_copy(own.at[i], dirs.at[block], recvs.at[block]).start()
        move(block, 1, x_dev, own.at[i])
        move(block, 2, y_dev, own.at[i])
        move(block, 0, partner, own.at[i])
        return carry
    lax.fori_loop(0, 5, begin, 0)

    def near(i, carry):
        block = x_dev * 5 + i
        landed(block, recvs.at[block])
        @pl.when(core == 0)
        def _():
            move(block, 2, y_dev)
        move(block, 0, partner)
        block = y_dev * 5 + i
        landed(block, recvs.at[block])
        @pl.when(core == 1)
        def _():
            move(block, 1, x_dev)
        move(block, 0, partner)
        return carry
    lax.fori_loop(0, 5, near, 0)

    def far(i, carry):
        block = far_dev * 5 + i
        landed(block, recvs.at[block])
        move(block, 0, partner)
        return carry
    lax.fori_loop(0, 5, far, 0)

    def finish(i, carry):
        block = me * 5 + i
        wait_bytes(dirs.at[block], recvs.at[block])
        for lane in range(3):
            landed(block, sends.at[block, lane])
        landed(x_dev * 5 + i, sends.at[x_dev * 5 + i, 0])
        landed(y_dev * 5 + i, sends.at[y_dev * 5 + i, 0])
        landed(far_dev * 5 + i, sends.at[far_dev * 5 + i, 0])
        @pl.when(core == 0)
        def _():
            landed(x_dev * 5 + i, sends.at[x_dev * 5 + i, 2])
        @pl.when(core == 1)
        def _():
            landed(y_dev * 5 + i, sends.at[y_dev * 5 + i, 1])
        for mask in (1, 3, 5, 7):
            block = flip(me, mask) * 5 + i
            landed(block, recvs.at[block])
        return carry
    lax.fori_loop(0, 5, finish, 0)


def gather_dirs(own, n_blocks):
    dma = pltpu.SemaphoreType.DMA
    return pl.pallas_call(
        gather_kernel,
        out_shape=jax.ShapeDtypeStruct((n_blocks, BLK, BLK), BF16),
        in_specs=[ANY],
        out_specs=ANY,
        scratch_shapes=[dma((n_blocks, 3)), dma((n_blocks,))],
        compiler_params=pltpu.CompilerParams(collective_id=1, has_side_effects=True),
        name='gather_dirs',
    )(own)


def apply_kernel(flipped, dirs, w, out):
    step = dirs[0, 0].astype(F32)
    step = step.T if flipped else step
    out[...] = w[...] - LEARN_RATE * (step + WEIGHT_DECAY * w[...])


def apply_update(w, dirs, flipped):
    rows, cols = w.shape
    grid = (-(-rows // BLK), -(-cols // BLK))
    if flipped:
        index = lambda i, j: (2 + i // 5, 2 * (i % 5) + j, 0, 0)
    else:
        index = lambda i, j: (i, j, 0, 0)
    return pl.pallas_call(
        functools.partial(apply_kernel, flipped),
        grid=grid,
        out_shape=jax.ShapeDtypeStruct(w.shape, F32),
        in_specs=[pl.BlockSpec((1, 1, BLK, BLK), index), pl.BlockSpec((BLK, BLK), lambda i, j: (i, j))],
        out_specs=pl.BlockSpec((BLK, BLK), lambda i, j: (i, j)),
        compiler_params=pltpu.CompilerParams(vmem_limit_bytes=VMEM_MAX),
        name='apply_update',
    )(dirs, w)


def solution(mesh):
    n_dev = mesh.shape['dp']

    def per_device(x_in, dy_mid, x_mid, dy_out, w_fc1, w_fc2, stat_left, stat_right, root_left, root_right, graft_sq, momentum):
        pieces = reduce_grads(x_in, dy_mid, x_mid, dy_out)
        new_left, new_right, new_sq, new_mom, own = block_update(n_dev, pieces, stat_left, stat_right, root_left, root_right, graft_sq, momentum)
        dirs = gather_dirs(own, n_dev * own.shape[0]).reshape(4, 10, BLK, BLK)
        new_w1 = apply_update(w_fc1, dirs, False)
        new_w2 = apply_update(w_fc2, dirs, True)
        return new_w1, new_w2, new_left, new_right, new_sq, new_mom

    row_spec = P('dp', None)
    rep_spec = P(None, None)
    tile_spec = P('dp', None, None)
    in_specs = (row_spec, row_spec, row_spec, row_spec, rep_spec, rep_spec, tile_spec, tile_spec, tile_spec, tile_spec, tile_spec, tile_spec)
    out_specs = (rep_spec, rep_spec, tile_spec, tile_spec, tile_spec, tile_spec)
    return jax.shard_map(per_device, mesh=mesh, in_specs=in_specs, out_specs=out_specs, check_vma=False)
```

```python
import functools

import jax
import jax.numpy as jnp
from jax import lax
from jax.experimental import pallas as pl
from jax.experimental.pallas import tpu as pltpu
from jax.sharding import PartitionSpec as P

STEP = 10
STAT_DECAY = 0.999
MOM_DECAY = 0.9
GRAFT_EPS = 1e-8
LEARN_RATE = 0.01
WEIGHT_DECAY = 1e-4
BIAS_CORR = 1.0 - STAT_DECAY ** STEP

MESH = pl.DeviceIdType.MESH
ANY = pl.BlockSpec(memory_space=pl.ANY)
BLK = 512
HALF = 256
STRIPS = 20
LAG = 4
HOPS, HOP_FROM, SEND_FROM = 3, 2, 0
EARLY = 3
ROWS_OF = (512, 384)
F32 = jnp.float32
BF16 = jnp.bfloat16
VMEM_MAX = 66 * 1000 * 1000


def flip(dev, mask):
    for bit in (1, 2, 4):
        if mask & bit:
            dev = dev + bit - 2 * bit * ((dev // bit) % 2)
    return dev


def send(src, dst, send_sem, recv_sem, dev):
    return pltpu.make_async_remote_copy(src_ref=src, dst_ref=dst, send_sem=send_sem, recv_sem=recv_sem, device_id=(dev,), device_id_type=MESH)


def wait_bytes(ref, sem):
    pltpu.make_async_copy(ref, ref, sem).wait()


def greet(devs):
    barrier = pltpu.get_barrier_semaphore()
    for dev in devs:
        pl.semaphore_signal(barrier, inc=1, device_id=(dev,), device_id_type=MESH)
    pl.semaphore_wait(barrier, len(devs))


def strip_of(pos):
    turn, grad = pos // 4, pos % 2
    return grad, jnp.where(grad == 0, turn, (3 * turn) % 5) + 5 * ((pos // 2) % 2)


def owner_of(grad, strip, part):
    in_chip = jnp.where(grad == 0, strip, 2 * (strip % 5) + part)
    return jnp.where(grad == 0, part, 2 + strip // 5), in_chip


def slot_at(chip, core, turn):
    return jnp.where((chip >= 2) & (core == 1), (turn + 1) % 5, turn)


def tile_at(chip, in_chip):
    strip = jnp.where(chip < 2, in_chip, 5 * (chip - 2) + in_chip // 2)
    return strip, jnp.where(chip < 2, chip, in_chip % 2)


def step_kernel(scale, x_in, dy_mid, x_mid, dy_out, root_left, root_right, graft_sq, momentum, stat_left, stat_right,
                first, second, home, new_left, new_right, new_sq, new_mom, own, pair, from_a, from_c, from_b, pair_a, pair_b,
                narrow, wide, out_buf, total, relay, piece_buf, state_buf, tile_a, tile_b,
                narrow_sem, wide_sem, pair_send, pair_recv, unit_sem, relay_sem, first_sem, second_sem, home_sem,
                piece_sem, state_sem, out_sem, dir_send, dir_recv, pass_send, pass_recv):
    me = lax.axis_index('dp')
    core = me % 2
    my_x, my_y = (me // 2) % 2, me // 4
    my_chip = me // 2
    partner, x_dev, y_dev = flip(me, 1), flip(me, 2), flip(me, 4)

    narrow_copies = [pltpu.make_async_copy(src, narrow.at[k], narrow_sem.at[k]) for k, src in enumerate((x_in, dy_out))]

    def load(job, pos, own_half):
        grad, strip = strip_of(pos)
        half = core if own_half else 1 - core
        off = pl.multiple_of(jnp.where(strip == 9, 9 * BLK, strip * BLK + half * HALF), HALF)
        slot = job % 3
        for k, src in enumerate((dy_mid, x_mid)):
            @pl.when(grad == k)
            def _():
                pltpu.make_async_copy(src.at[:, pl.ds(off, HALF)], wide.at[slot], wide_sem.at[slot]).start()

    def load_job(job):
        @pl.when((job % 2 == 1) & (job < 39))
        def _():
            load(job, (job + 1) // 2, False)
        @pl.when(job % 2 == 0)
        def _():
            load(job, job // 2 - 1, True)
        @pl.when(job == 39)
        def _():
            load(job, 19, True)

    narrow_copies[0].start()
    load(0, 0, False)
    load(1, 1, False)
    narrow_copies[1].start()
    greet([partner, x_dev, flip(me, 3), y_dev, flip(me, 5)])

    def product(pos, slot):
        grad, _ = strip_of(pos)
        return lax.dot_general(narrow[grad], wide[slot], (((0,), (0,)), ((), ())), preferred_element_type=F32)

    def given(pos):
        grad, strip = strip_of(pos)
        return (strip != 9) | (grad != core)

    def kept(pos):
        grad, strip = strip_of(pos)
        return (strip != 9) | (grad == core)

    def give(pos, job):
        slot = job % 3
        wait_bytes(wide.at[slot], wide_sem.at[slot])

        @pl.when(given(pos))
        def _():
            @pl.when(pos >= 2)
            def _():
                wait_bytes(out_buf.at[pos % 2], pair_send.at[pos % 2])
            out_buf[pos % 2] = product(pos, slot)
            send(out_buf.at[pos % 2], total.at[pos], pair_send.at[pos % 2], pair_recv.at[pos], partner).start()

    def unit(pos, part):
        grad, strip = strip_of(pos)
        chip, in_chip = owner_of(grad, strip, part)
        own_core = in_chip // 5
        odd_one = in_chip % 5 == 2
        x_first = jnp.where(odd_one, chip % 2 == 1, core == 0)
        dif_x, dif_y = my_x != chip % 2, my_y != chip // 2
        slot = jnp.where(odd_one & (chip % 2 == 0), 10 + in_chip // 5, in_chip)
        return dict(idx=in_chip % 5, own_core=own_core, half=jnp.where(strip == 9, 0, core), x_first=x_first,
                    near=(dif_x & ~dif_y & x_first) | (dif_y & ~dif_x & ~x_first),
                    second=(dif_y & ~dif_x & x_first) | (dif_x & ~dif_y & ~x_first),
                    far=dif_x & dif_y, mine=~dif_x & ~dif_y,
                    rows=pl.ds(0, ROWS_OF[part]), src=total.at[pos, pl.ds(part * 512, ROWS_OF[part]), :],
                    sem=unit_sem.at[pos * 2 + part], dest=chip * 2 + own_core, slot=slot)

    def keep(pos, job):
        slot = job % 3
        wait_bytes(wide.at[slot], wide_sem.at[slot])

        @pl.when(kept(pos))
        def _():
            wait_bytes(total.at[pos], pair_recv.at[pos])
            total[pos] = total[pos] + product(pos, slot)
            for part in (0, 1):
                u = unit(pos, part)

                @pl.when(u['near'])
                def _():
                    send(u['src'], first.at[u['idx'], u['half'], u['rows'], :], u['sem'], first_sem.at[u['idx'], u['half']], u['dest']).start()

                @pl.when(u['far'] & u['x_first'])
                def _():
                    send(u['src'], relay.at[u['slot'], u['rows'], :], u['sem'], relay_sem.at[u['slot']], x_dev).start()

                @pl.when(u['far'] & ~u['x_first'])
                def _():
                    send(u['src'], relay.at[u['slot'], u['rows'], :], u['sem'], relay_sem.at[u['slot']], y_dev).start()

                @pl.when(u['mine'] & (u['own_core'] == core))
                def _():
                    pltpu.make_async_copy(u['src'], home.at[u['idx'], u['half'], u['rows'], :], u['sem']).start()

                @pl.when(u['mine'] & (u['own_core'] != core))
                def _():
                    send(u['src'], home.at[u['idx'], u['half'], u['rows'], :], u['sem'], home_sem.at[u['idx']], partner).start()

    narrow_copies[0].wait()
    load(2, 0, True)
    give(0, 0)
    narrow_copies[1].wait()

    def hop(pos, carry):
        @pl.when(kept(pos))
        def _():
            for part in (0, 1):
                u = unit(pos, part)

                @pl.when(u['second'])
                def _():
                    here = pl.ds(part * 512, ROWS_OF[part])
                    wait_bytes(relay.at[u['slot'], u['rows'], :], relay_sem.at[u['slot']])
                    total[pos, here, :] = total[pos, here, :] + relay[u['slot'], u['rows'], :]
                    send(u['src'], second.at[u['idx'], u['half'], u['rows'], :], u['sem'], second_sem.at[u['idx'], u['half']], u['dest']).start()
        return carry

    def step(pos, carry):
        job = 2 * pos - 1
        load_job(job + 2)
        give(pos, job)

        @pl.when(pos < 19)
        def _():
            load_job(job + 3)
        keep(pos - 1, job + 1)

        @pl.when(pos > LAG)
        def _():
            hop(pos - 1 - LAG, 0)
        return carry
    lax.fori_loop(1, STRIPS, step, 0)
    keep(19, 39)

    def fetch_state(turn):
        idx = slot_at(my_chip, core, turn)
        for k, src in enumerate((root_left, root_right, graft_sq, momentum, stat_left, stat_right)):
            pltpu.make_async_copy(src.at[idx], state_buf.at[k], state_sem.at[k]).start()
    fetch_state(0)

    for slot in (0, 1):
        wait_bytes(out_buf.at[slot], pair_send.at[slot])

    row = lax.broadcasted_iota(jnp.int32, (BLK, BLK), 0)
    col = lax.broadcasted_iota(jnp.int32, (BLK, BLK), 1)
    on_first = my_chip < 2
    chunk = 256

    def split(value, at):
        high = value.astype(BF16)
        narrow[1, pl.ds(at * BLK, BLK), pl.ds(0, BLK)] = high
        narrow[1, pl.ds((at + 1) * BLK, BLK), pl.ds(0, BLK)] = (value - high.astype(F32)).astype(BF16)

    def times(value, at):
        high = value.astype(BF16)
        low = (value - high.astype(F32)).astype(BF16)
        dot = functools.partial(jnp.dot, preferred_element_type=F32)
        b_high = narrow[1, pl.ds(at * BLK, BLK), pl.ds(0, BLK)]
        b_low = narrow[1, pl.ds((at + 1) * BLK, BLK), pl.ds(0, BLK)]
        return dot(high, b_high) + (dot(high, b_low) + dot(low, b_high))

    def leave(turn):
        tall = tile_at(my_chip, 5 * core + slot_at(my_chip, core, turn))[1]
        for part in (0, 1):
            rows = pl.ds(0, ROWS_OF[part])

            @pl.when(tall == part)
            def _():
                src = narrow.at[0, pl.ds(pl.multiple_of(turn * BLK, BLK), ROWS_OF[part]), pl.ds(0, BLK)]
                pltpu.make_async_copy(src, own.at[turn, rows, :], dir_send.at[0, turn]).start()
                for k, (dev_a, dev_b) in enumerate(((x_dev, y_dev), (y_dev, x_dev))):
                    @pl.when((core == k) & (turn < EARLY))
                    def _():
                        send(src, from_a.at[turn, rows, :], dir_send.at[2, turn], dir_recv.at[1, turn], dev_a).start()

                    @pl.when((core == k) & (turn >= EARLY))
                    def _():
                        send(src, from_c.at[turn - EARLY, rows, :], dir_send.at[2, turn], dir_recv.at[1, turn], dev_a).start()

                    @pl.when(core == k)
                    def _():
                        send(src, from_b.at[turn, rows, :], dir_send.at[3, turn], dir_recv.at[2, turn], dev_b).start()
                send(src, pair.at[turn, rows, :], dir_send.at[1, turn], dir_recv.at[0, turn], partner).start()

    def block(turn, carry):
        for k in range(HOPS):
            pos = STRIPS - 1 - LAG + HOPS * (turn - HOP_FROM) + k

            @pl.when((turn >= HOP_FROM) & (pos < STRIPS))
            def _():
                hop(pos, 0)
        idx = slot_at(my_chip, core, turn)
        in_chip = 5 * core + idx
        strip, tall = tile_at(my_chip, in_chip)
        for half in (0, 1):
            source = jnp.where(strip == 9, jnp.where(on_first, 0, 1), half)
            for part in (0, 1):
                rows = pl.ds(0, ROWS_OF[part])

                @pl.when((tall == part) & ((strip < 9) | (half == 0)))
                def _():
                    wait_bytes(first.at[idx, half, rows, :], first_sem.at[idx, half])
                    wait_bytes(second.at[idx, half, rows, :], second_sem.at[idx, half])

                    @pl.when(source != core)
                    def _():
                        wait_bytes(home.at[idx, half, rows, :], home_sem.at[idx])

                    @pl.when(source == core)
                    def _():
                        for grad in (0, 1):
                            @pl.when(on_first == (grad == 0))
                            def _():
                                turn5 = strip % 5 if grad == 0 else (2 * (strip % 5)) % 5
                                pos = 4 * turn5 + 2 * (strip // 5) + grad
                                wait_bytes(home.at[idx, half, rows, :], unit_sem.at[pos * 2 + part])
        for k, src in enumerate((home, first, second)):
            pltpu.make_async_copy(src.at[idx], piece_buf.at[k], piece_sem.at[k]).start()
        for k, src in enumerate((home, first, second)):
            wait_bytes(piece_buf.at[k], piece_sem.at[k])
        n_rows = jnp.where(tall == 0, 512, 384)
        n_cols = jnp.where(strip == 9, 256, 512)
        for half in (0, 1):
            here = pl.ds(half * HALF, HALF)
            value = ((piece_buf[0, half] + piece_buf[1, half]) + piece_buf[2, half]) * scale
            tile_a[:, here] = jnp.where((row[:, :HALF] < n_rows) & (col[:, :HALF] + half * HALF < n_cols), value, 0.0)

        @pl.when(on_first)
        def _():
            tile_b[...] = tile_a[...]

        @pl.when(~on_first)
        def _():
            tile_b[...] = tile_a[...].T
        for k in range(6):
            wait_bytes(state_buf.at[k], state_sem.at[k])
        split(tile_b[...], 0)
        split(state_buf[1], 2)
        nat_rows = jnp.where(on_first, n_rows, n_cols)
        nat_cols = jnp.where(on_first, n_cols, n_rows)

        def rows_step(r, sums):
            here = pl.ds(pl.multiple_of(r * chunk, chunk), chunk)
            pre = times(times(state_buf[0, here, :], 0), 2)
            pre = jnp.where((row[:chunk] + r * chunk < nat_rows) & (col[:chunk] < nat_cols), pre, 0.0)
            tile_a[here, :] = pre
            grad = tile_b[here, :]
            sq_now = STAT_DECAY * state_buf[2, here, :] + (1.0 - STAT_DECAY) * grad * grad
            state_buf[2, here, :] = sq_now
            graft = grad / (jnp.sqrt(sq_now / BIAS_CORR) + GRAFT_EPS)
            return sums[0] + jnp.sum(graft * graft, keepdims=True), sums[1] + jnp.sum(pre * pre, keepdims=True)
        zero = jnp.zeros((1, 1), F32)
        graft_sum, pre_sum = lax.fori_loop(0, BLK // chunk, rows_step, (zero, zero))
        ratio = jnp.sqrt(graft_sum) / jnp.sqrt(pre_sum)
        state_buf[3] = MOM_DECAY * state_buf[3] + tile_a[...] * ratio
        dirs = narrow.at[0, pl.ds(pl.multiple_of(turn * BLK, BLK), BLK), pl.ds(0, BLK)]

        @pl.when(on_first)
        def _():
            dirs[...] = state_buf[3].astype(BF16)

        @pl.when(~on_first)
        def _():
            dirs[...] = state_buf[3].T.astype(BF16)

        @pl.when(turn == SEND_FROM)
        def _():
            for k in range(SEND_FROM):
                leave(k)

        @pl.when(turn >= SEND_FROM)
        def _():
            leave(turn)

        def stats_step(r, carry):
            here = pl.ds(pl.multiple_of(r * chunk, chunk), chunk)
            high = narrow[1, pl.ds(0, BLK), pl.ds(0, BLK)]
            low = narrow[1, pl.ds(BLK, BLK), pl.ds(0, BLK)]
            dot = functools.partial(lax.dot_general, preferred_element_type=F32)
            nt, tn = (((1,), (1,)), ((), ())), (((0,), (0,)), ((), ()))
            a_high = narrow[1, here, pl.ds(0, BLK)]
            a_low = narrow[1, pl.ds(pl.multiple_of(BLK + r * chunk, chunk), chunk), pl.ds(0, BLK)]
            state_buf[4, here, :] = STAT_DECAY * state_buf[4, here, :] + (1.0 - STAT_DECAY) * (
                dot(a_high, high, nt) + (dot(a_high, low, nt) + dot(a_low, high, nt)))
            b_high = narrow[1, pl.ds(0, BLK), here]
            b_low = narrow[1, pl.ds(BLK, BLK), here]
            state_buf[5, here, :] = STAT_DECAY * state_buf[5, here, :] + (1.0 - STAT_DECAY) * (
                dot(b_high, high, tn) + (dot(b_high, low, tn) + dot(b_low, high, tn)))
            return carry
        lax.fori_loop(0, BLK // chunk, stats_step, 0)
        for k, dst in enumerate((new_sq, new_mom, new_left, new_right)):
            pltpu.make_async_copy(state_buf.at[2 + k], dst.at[idx], out_sem.at[k]).start()
        for k in range(4):
            wait_bytes(state_buf.at[2 + k], out_sem.at[k])

        @pl.when(turn < 4)
        def _():
            fetch_state(turn + 1)
        return carry
    lax.fori_loop(0, 5, block, 0)

    def drain(pos, carry):
        @pl.when(kept(pos))
        def _():
            for part in (0, 1):
                u = unit(pos, part)

                @pl.when(~(u['mine'] & (u['own_core'] == core)))
                def _():
                    wait_bytes(u['src'], u['sem'])
        return carry
    lax.fori_loop(0, STRIPS, drain, 0)

    x_chip, y_chip = x_dev // 2, y_dev // 2
    a_chip, b_chip = jnp.where(core == 0, x_chip, y_chip), jnp.where(core == 0, y_chip, x_chip)

    def tall_of(chip, its_core, turn):
        return tile_at(chip, 5 * its_core + slot_at(chip, its_core, turn))[1]

    def hand_on(turn, carry):
        for part in (0, 1):
            rows = pl.ds(0, ROWS_OF[part])
            ref = own.at[turn, rows, :]

            @pl.when(tall_of(a_chip, core, turn) == part)
            def _():
                wait_bytes(ref, dir_recv.at[1, turn])

                @pl.when(turn < EARLY)
                def _():
                    send(from_a.at[turn, rows, :], pair_a.at[turn, rows, :], pass_send.at[0, turn], pass_recv.at[0, turn], partner).start()

                @pl.when(turn >= EARLY)
                def _():
                    send(from_c.at[turn - EARLY, rows, :], pair_a.at[turn, rows, :], pass_send.at[0, turn], pass_recv.at[0, turn], partner).start()

            @pl.when(tall_of(b_chip, core, turn) == part)
            def _():
                wait_bytes(ref, dir_recv.at[2, turn])
                send(from_b.at[turn, rows, :], pair_b.at[turn, rows, :], pass_send.at[1, turn], pass_recv.at[1, turn], partner).start()
        return carry
    lax.fori_loop(0, 5, hand_on, 0)

    def dirs_done(turn, carry):
        for part in (0, 1):
            ref = own.at[turn, pl.ds(0, ROWS_OF[part]), :]

            @pl.when(tall_of(my_chip, core, turn) == part)
            def _():
                for lane in range(4):
                    wait_bytes(ref, dir_send.at[lane, turn])
            for sem, chip, its_core in ((dir_recv.at[0, turn], my_chip, 1 - core), (pass_send.at[0, turn], a_chip, core),
                                        (pass_send.at[1, turn], b_chip, core), (pass_recv.at[0, turn], b_chip, 1 - core),
                                        (pass_recv.at[1, turn], a_chip, 1 - core)):
                @pl.when(tall_of(chip, its_core, turn) == part)
                def _():
                    wait_bytes(ref, sem)
        return carry
    lax.fori_loop(0, 5, dirs_done, 0)


def step_blocks(n_dev, x_in, dy_mid, x_mid, dy_out, root_left, root_right, graft_sq, momentum, stat_left, stat_right):
    tokens, n_model = x_in.shape
    piece = jax.ShapeDtypeStruct((5, 2, BLK, HALF), F32)
    tile = jax.ShapeDtypeStruct((5, BLK, BLK), F32)
    dirs, early, late = (jax.ShapeDtypeStruct((k, BLK, BLK), BF16) for k in (5, EARLY, 5 - EARLY))
    dma = pltpu.SemaphoreType.DMA
    outs = pl.pallas_call(
        functools.partial(step_kernel, 1.0 / n_dev),
        out_shape=(piece, piece, piece, tile, tile, tile, tile, dirs, dirs, early, late, dirs, dirs, dirs),
        in_specs=[ANY] * 10,
        out_specs=(ANY,) * 14,
        scratch_shapes=[
            pltpu.VMEM((2, tokens, n_model), BF16),
            pltpu.VMEM((3, tokens, HALF), BF16),
            pltpu.VMEM((2, n_model, HALF), F32),
            pltpu.VMEM((STRIPS, n_model, HALF), F32),
            pltpu.VMEM((12, BLK, HALF), F32),
            pltpu.VMEM((3, 2, BLK, HALF), F32),
            pltpu.VMEM((6, BLK, BLK), F32),
            pltpu.VMEM((BLK, BLK), F32),
            pltpu.VMEM((BLK, BLK), F32),
            dma((2,)), dma((3,)), dma((2,)), dma((STRIPS,)), dma((2 * STRIPS,)), dma((12,)), dma((5, 2)), dma((5, 2)), dma((5,)),
            dma((3,)), dma((6,)), dma((4,)), dma((4, 5)), dma((3, 5)), dma((2, 5)), dma((2, 5)),
        ],
        compiler_params=pltpu.CompilerParams(collective_id=0, has_side_effects=True, vmem_limit_bytes=VMEM_MAX),
        name='step_blocks',
    )(x_in, dy_mid, x_mid, dy_out, root_left, root_right, graft_sq, momentum, stat_left, stat_right)
    return outs[3:]


def pass_kernel(*refs):
    for src, dst in zip(refs[:4], refs[4:]):
        dst[...] = src[...]


def pass_on(states):
    spec = pl.BlockSpec((1, BLK, BLK), lambda i: (i, 0, 0))
    return pl.pallas_call(
        pass_kernel,
        grid=(states[0].shape[0],),
        out_shape=tuple(jax.ShapeDtypeStruct(x.shape, x.dtype) for x in states),
        in_specs=[spec] * 4,
        out_specs=(spec,) * 4,
        compiler_params=pltpu.CompilerParams(vmem_limit_bytes=VMEM_MAX),
        cost_estimate=pl.CostEstimate(flops=10 ** 10, bytes_accessed=42 * 10 ** 6, transcendentals=0),
        name='pass_on',
    )(*states)


BUFS, AHEAD = 4, 3


def apply_kernel(places, *refs):
    n_src = len(places)
    srcs, (w1, w2) = refs[:n_src], refs[n_src:n_src + 2]
    outs = refs[-8:-6]
    dir_buf, w_buf, o_buf, dir_sem, w_sem, o_sem = refs[-6:]
    me = lax.axis_index('dp')
    core, my_chip = me % 2, me // 2
    x_chip, y_chip, far_chip = flip(me, 2) // 2, flip(me, 4) // 2, flip(me, 6) // 2
    a_chip, b_chip = jnp.where(core == 0, x_chip, y_chip), jnp.where(core == 0, y_chip, x_chip)
    chips = dict(own=my_chip, a=a_chip, b=b_chip, far=far_chip)
    counts = [src.shape[0] for src in srcs]
    starts = [sum(counts[:k]) for k in range(n_src)]
    n_tiles = sum(counts)

    def tile(n):
        which, spot, turn, chip, its_core = 0, n, n + places[0][2], chips[places[0][0]], core if places[0][1] else 1 - core
        for k, (name, same, begin) in enumerate(places):
            here = n >= starts[k]
            which = jnp.where(here, k, which)
            spot = jnp.where(here, n - starts[k], spot)
            turn = jnp.where(here, n - starts[k] + begin, turn)
            chip = jnp.where(here, chips[name], chip)
            its_core = jnp.where(here, core if same else 1 - core, its_core)
        strip, tall = tile_at(chip, 5 * its_core + slot_at(chip, its_core, turn))
        return which, spot, chip, strip, tall

    def window(n, do):
        _, _, chip, strip, tall = tile(n)
        for tall_k in (0, 1):
            for last in (0, 1):
                big, small = ROWS_OF[tall_k], (512, 256)[last]
                at = pl.multiple_of(strip * BLK, BLK)
                here = (tall == tall_k) & ((strip == 9) == (last == 1))

                @pl.when(here & (chip < 2))
                def _():
                    do(0, (pl.ds(tall_k * BLK, big), pl.ds(at, small)), (pl.ds(0, big), pl.ds(0, small)))

                @pl.when(here & (chip >= 2))
                def _():
                    do(1, (pl.ds(at, small), pl.ds(tall_k * BLK, big)), (pl.ds(0, small), pl.ds(0, big)))

    def load(n):
        which, turn, _, _, _ = tile(n)
        slot = n % BUFS
        for k, src in enumerate(srcs):
            @pl.when(which == k)
            def _():
                pltpu.make_async_copy(src.at[turn], dir_buf.at[slot], dir_sem.at[slot]).start()
        window(n, lambda k, at, view: pltpu.make_async_copy((w1, w2)[k].at[at], w_buf.at[slot].at[view], w_sem.at[slot]).start())

    def load_wait(n):
        slot = n % BUFS
        wait_bytes(dir_buf.at[slot], dir_sem.at[slot])
        window(n, lambda k, at, view: wait_bytes(w_buf.at[slot].at[view], w_sem.at[slot]))

    def store_wait(n):
        slot = n % BUFS
        window(n, lambda k, at, view: wait_bytes(o_buf.at[slot].at[view], o_sem.at[slot]))

    for n in range(AHEAD):
        load(n)

    def step(n, carry):
        slot = n % BUFS

        @pl.when(n + AHEAD < n_tiles)
        def _():
            load(n + AHEAD)
        load_wait(n)

        @pl.when(n >= BUFS)
        def _():
            store_wait(n - BUFS)
        chip = tile(n)[2]

        @pl.when(chip < 2)
        def _():
            o_buf[slot] = w_buf[slot] - LEARN_RATE * (dir_buf[slot].astype(F32) + WEIGHT_DECAY * w_buf[slot])

        @pl.when(chip >= 2)
        def _():
            o_buf[slot] = w_buf[slot] - LEARN_RATE * (dir_buf[slot].astype(F32).T + WEIGHT_DECAY * w_buf[slot])
        window(n, lambda k, at, view: pltpu.make_async_copy(o_buf.at[slot].at[view], outs[k].at[at], o_sem.at[slot]).start())
        return carry
    lax.fori_loop(0, n_tiles, step, 0)
    for n in range(n_tiles - BUFS, n_tiles):
        store_wait(n)


def apply_update(places, srcs, w1, w2, partial=()):
    dma = pltpu.SemaphoreType.DMA
    n_in = len(srcs) + 2
    share = sum(src.shape[0] for src in srcs) / 40
    return pl.pallas_call(
        functools.partial(apply_kernel, places),
        out_shape=(jax.ShapeDtypeStruct(w1.shape, F32), jax.ShapeDtypeStruct(w2.shape, F32)),
        in_specs=[ANY] * (n_in + len(partial)),
        out_specs=(ANY, ANY),
        scratch_shapes=[
            pltpu.VMEM((BUFS, BLK, BLK), BF16), pltpu.VMEM((BUFS, BLK, BLK), F32), pltpu.VMEM((BUFS, BLK, BLK), F32),
            dma((BUFS,)), dma((BUFS,)), dma((BUFS,)),
        ],
        input_output_aliases={n_in: 0, n_in + 1: 1} if partial else {},
        compiler_params=pltpu.CompilerParams(vmem_limit_bytes=VMEM_MAX),
        cost_estimate=pl.CostEstimate(flops=int(share * 20 * 10 ** 9), bytes_accessed=int(share * 88 * 10 ** 6), transcendentals=0),
        name='apply_update',
    )(*srcs, w1, w2, *partial)


def solution(mesh):
    n_dev = mesh.shape['dp']
    swap = [(i, i ^ 1) for i in range(n_dev)]
    onward = [(i, i ^ (4 if i % 2 == 0 else 2)) for i in range(n_dev)]

    def per_device(x_in, dy_mid, x_mid, dy_out, w_fc1, w_fc2, stat_left, stat_right, root_left, root_right, graft_sq, momentum):
        *states, own, pair, from_a, from_c, from_b, pair_a, pair_b = step_blocks(
            n_dev, x_in, dy_mid, x_mid, dy_out, root_left, root_right, graft_sq, momentum, stat_left, stat_right)
        far = lax.ppermute(from_a, 'dp', onward)
        far_late = lax.ppermute(from_c, 'dp', onward)
        near = (('own', True, 0), ('own', False, 0), ('a', True, 0), ('a', True, EARLY), ('b', True, 0), ('b', False, 0), ('a', False, 0))
        partial = apply_update(near, (own, pair, from_a, from_c, from_b, pair_a, pair_b), w_fc1, w_fc2)
        far, partial, *states = lax.optimization_barrier((far, partial, *states))
        pair_far = lax.ppermute(far, 'dp', swap)
        new_left, new_right, new_sq, new_mom = pass_on(states)
        partial = apply_update((('far', True, 0), ('far', False, 0)), (far, pair_far), w_fc1, w_fc2, partial)
        pair_far_late = lax.ppermute(far_late, 'dp', swap)
        new_w1, new_w2 = apply_update((('far', True, EARLY), ('far', False, EARLY)), (far_late, pair_far_late), w_fc1, w_fc2, partial)
        return new_w1, new_w2, new_left, new_right, new_sq, new_mom

    row_spec = P('dp', None)
    rep_spec = P(None, None)
    tile_spec = P('dp', None, None)
    in_specs = (row_spec, row_spec, row_spec, row_spec, rep_spec, rep_spec, tile_spec, tile_spec, tile_spec, tile_spec, tile_spec, tile_spec)
    out_specs = (rep_spec, rep_spec, tile_spec, tile_spec, tile_spec, tile_spec)
    return jax.shard_map(per_device, mesh=mesh, in_specs=in_specs, out_specs=out_specs, check_vma=False)
```

```python
import functools

import jax
import jax.numpy as jnp
from jax import lax
from jax.experimental import pallas as pl
from jax.experimental.pallas import tpu as pltpu
from jax.sharding import PartitionSpec as P


STEP = 10
STAT_DECAY = 0.999
MOM_DECAY = 0.9
GRAFT_EPS = 1e-8
LEARN_RATE = 0.01
WEIGHT_DECAY = 1e-4
BIAS_CORR = 1.0 - STAT_DECAY ** STEP

MESH = pl.DeviceIdType.MESH
ANY = pl.BlockSpec(memory_space=pl.ANY)
BLK = 512
HALF = 256
STRIPS = 20
LAG = 4
HOPS, HOP_FROM, SEND_FROM = 3, 2, 0
EARLY = 3
ROWS_OF = (512, 384)
F32 = jnp.float32
BF16 = jnp.bfloat16
VMEM_MAX = 66 * 1000 * 1000


def flip(dev, mask):
    for bit in (1, 2, 4):
        if mask & bit:
            dev = dev + bit - 2 * bit * ((dev // bit) % 2)
    return dev


def send(src, dst, send_sem, recv_sem, dev):
    return pltpu.make_async_remote_copy(src_ref=src, dst_ref=dst, send_sem=send_sem, recv_sem=recv_sem, device_id=(dev,), device_id_type=MESH)


def wait_bytes(ref, sem):
    pltpu.make_async_copy(ref, ref, sem).wait()


def greet(devs):
    barrier = pltpu.get_barrier_semaphore()
    for dev in devs:
        pl.semaphore_signal(barrier, inc=1, device_id=(dev,), device_id_type=MESH)
    pl.semaphore_wait(barrier, len(devs))


def strip_of(pos):
    turn, grad = pos // 4, pos % 2
    return grad, jnp.where(grad == 0, turn, (3 * turn) % 5) + 5 * ((pos // 2) % 2)


def owner_of(grad, strip, part):
    in_chip = jnp.where(grad == 0, strip, 2 * (strip % 5) + part)
    return jnp.where(grad == 0, part, 2 + strip // 5), in_chip


def slot_at(chip, core, turn):
    return jnp.where((chip >= 2) & (core == 1), (turn + 1) % 5, turn)


def tile_at(chip, in_chip):
    strip = jnp.where(chip < 2, in_chip, 5 * (chip - 2) + in_chip // 2)
    return strip, jnp.where(chip < 2, chip, in_chip % 2)


def step_kernel(scale, x_in, dy_mid, x_mid, dy_out, root_left, root_right, graft_sq, momentum, stat_left, stat_right,
                first, second, home, new_left, new_right, new_sq, new_mom, own, pair, from_a, from_c, from_b, pair_a, pair_b,
                narrow, wide, out_buf, total, relay, piece_buf, state_buf, tile_a, tile_b,
                narrow_sem, wide_sem, pair_send, pair_recv, unit_sem, relay_sem, first_sem, second_sem, home_sem,
                piece_sem, state_sem, out_sem, dir_send, dir_recv, pass_send, pass_recv):
    me = lax.axis_index('dp')
    core = me % 2
    my_x, my_y = (me // 2) % 2, me // 4
    my_chip = me // 2
    partner, x_dev, y_dev = flip(me, 1), flip(me, 2), flip(me, 4)

    narrow_copies = [pltpu.make_async_copy(src, narrow.at[k], narrow_sem.at[k]) for k, src in enumerate((x_in, dy_out))]

    def load(job, pos, own_half):
        grad, strip = strip_of(pos)
        half = core if own_half else 1 - core
        off = pl.multiple_of(jnp.where(strip == 9, 9 * BLK, strip * BLK + half * HALF), HALF)
        slot = job % 3
        for k, src in enumerate((dy_mid, x_mid)):
            @pl.when(grad == k)
            def _():
                pltpu.make_async_copy(src.at[:, pl.ds(off, HALF)], wide.at[slot], wide_sem.at[slot]).start()

    def load_job(job):
        @pl.when((job % 2 == 1) & (job < 39))
        def _():
            load(job, (job + 1) // 2, False)

        @pl.when(job % 2 == 0)
        def _():
            load(job, job // 2 - 1, True)

        @pl.when(job == 39)
        def _():
            load(job, 19, True)

    narrow_copies[0].start()
    load(0, 0, False)
    load(1, 1, False)
    greet([partner, x_dev, flip(me, 3), y_dev, flip(me, 5)])

    def product(pos, slot):
        grad, _ = strip_of(pos)
        return lax.dot_general(narrow[grad], wide[slot], (((0,), (0,)), ((), ())), preferred_element_type=F32)

    def given(pos):
        grad, strip = strip_of(pos)
        return (strip != 9) | (grad != core)

    def kept(pos):
        grad, strip = strip_of(pos)
        return (strip != 9) | (grad == core)

    def give(pos, job):
        slot = job % 3
        wait_bytes(wide.at[slot], wide_sem.at[slot])

        @pl.when(given(pos))
        def _():
            @pl.when(pos >= 2)
            def _():
                wait_bytes(out_buf.at[pos % 2], pair_send.at[pos % 2])

            out_buf[pos % 2] = product(pos, slot)
            send(out_buf.at[pos % 2], total.at[pos], pair_send.at[pos % 2], pair_recv.at[pos], partner).start()

    def unit(pos, part):
        grad, strip = strip_of(pos)
        chip, in_chip = owner_of(grad, strip, part)
        own_core = in_chip // 5
        odd_one = in_chip % 5 == 2
        x_first = jnp.where(odd_one, chip % 2 == 1, core == 0)
        dif_x, dif_y = my_x != chip % 2, my_y != chip // 2
        slot = jnp.where(odd_one & (chip % 2 == 0), 10 + in_chip // 5, in_chip)
        return dict(idx=in_chip % 5, own_core=own_core, half=jnp.where(strip == 9, 0, core), x_first=x_first,
                    near=(dif_x & ~dif_y & x_first) | (dif_y & ~dif_x & ~x_first),
                    second=(dif_y & ~dif_x & x_first) | (dif_x & ~dif_y & ~x_first),
                    far=dif_x & dif_y, mine=~dif_x & ~dif_y,
                    rows=pl.ds(0, ROWS_OF[part]), src=total.at[pos, pl.ds(part * 512, ROWS_OF[part]), :],
                    sem=unit_sem.at[pos * 2 + part], dest=chip * 2 + own_core, slot=slot)

    def keep(pos, job):
        slot = job % 3
        wait_bytes(wide.at[slot], wide_sem.at[slot])

        @pl.when(kept(pos))
        def _():
            wait_bytes(total.at[pos], pair_recv.at[pos])
            total[pos] = total[pos] + product(pos, slot)
            for part in (0, 1):
                u = unit(pos, part)

                @pl.when(u['near'])
                def _():
                    send(u['src'], first.at[u['idx'], u['half'], u['rows'], :], u['sem'], first_sem.at[u['idx'], u['half']], u['dest']).start()

                @pl.when(u['far'] & u['x_first'])
                def _():
                    send(u['src'], relay.at[u['slot'], u['rows'], :], u['sem'], relay_sem.at[u['slot']], x_dev).start()

                @pl.when(u['far'] & ~u['x_first'])
                def _():
                    send(u['src'], relay.at[u['slot'], u['rows'], :], u['sem'], relay_sem.at[u['slot']], y_dev).start()

                @pl.when(u['mine'] & (u['own_core'] == core))
                def _():
                    pltpu.make_async_copy(u['src'], home.at[u['idx'], u['half'], u['rows'], :], u['sem']).start()

                @pl.when(u['mine'] & (u['own_core'] != core))
                def _():
                    send(u['src'], home.at[u['idx'], u['half'], u['rows'], :], u['sem'], home_sem.at[u['idx']], partner).start()

    narrow_copies[0].wait()
    narrow_copies[1].start()
    load(2, 0, True)
    give(0, 0)
    narrow_copies[1].wait()

    def hop(pos, carry):
        @pl.when(kept(pos))
        def _():
            for part in (0, 1):
                u = unit(pos, part)

                @pl.when(u['second'])
                def _():
                    here = pl.ds(part * 512, ROWS_OF[part])
                    wait_bytes(relay.at[u['slot'], u['rows'], :], relay_sem.at[u['slot']])
                    total[pos, here, :] = total[pos, here, :] + relay[u['slot'], u['rows'], :]
                    send(u['src'], second.at[u['idx'], u['half'], u['rows'], :], u['sem'], second_sem.at[u['idx'], u['half']], u['dest']).start()

        return carry

    def step(pos, carry):
        job = 2 * pos - 1
        load_job(job + 2)
        give(pos, job)

        @pl.when(pos < 19)
        def _():
            load_job(job + 3)

        keep(pos - 1, job + 1)

        @pl.when(pos > LAG)
        def _():
            hop(pos - 1 - LAG, 0)

        return carry

    lax.fori_loop(1, STRIPS, step, 0)
    keep(19, 39)

    def fetch_state(turn):
        idx = slot_at(my_chip, core, turn)
        for k, src in enumerate((root_left, root_right, graft_sq, momentum, stat_left, stat_right)):
            pltpu.make_async_copy(src.at[idx], state_buf.at[k], state_sem.at[k]).start()

    fetch_state(0)

    for slot in (0, 1):
        wait_bytes(out_buf.at[slot], pair_send.at[slot])

    row = lax.broadcasted_iota(jnp.int32, (BLK, BLK), 0)
    col = lax.broadcasted_iota(jnp.int32, (BLK, BLK), 1)
    on_first = my_chip < 2
    chunk = 256

    def split(value, at):
        high = value.astype(BF16)
        narrow[1, pl.ds(at * BLK, BLK), pl.ds(0, BLK)] = high
        narrow[1, pl.ds((at + 1) * BLK, BLK), pl.ds(0, BLK)] = (value - high.astype(F32)).astype(BF16)

    def times(value, at):
        high = value.astype(BF16)
        low = (value - high.astype(F32)).astype(BF16)
        dot = functools.partial(jnp.dot, preferred_element_type=F32)
        b_high = narrow[1, pl.ds(at * BLK, BLK), pl.ds(0, BLK)]
        b_low = narrow[1, pl.ds((at + 1) * BLK, BLK), pl.ds(0, BLK)]
        return dot(high, b_high) + (dot(high, b_low) + dot(low, b_high))

    def leave(turn):
        tall = tile_at(my_chip, 5 * core + slot_at(my_chip, core, turn))[1]
        for part in (0, 1):
            rows = pl.ds(0, ROWS_OF[part])

            @pl.when(tall == part)
            def _():
                src = narrow.at[0, pl.ds(pl.multiple_of(turn * BLK, BLK), ROWS_OF[part]), pl.ds(0, BLK)]
                pltpu.make_async_copy(src, own.at[turn, rows, :], dir_send.at[0, turn]).start()
                for k, (dev_a, dev_b) in enumerate(((x_dev, y_dev), (y_dev, x_dev))):
                    @pl.when((core == k) & (turn < EARLY))
                    def _():
                        send(src, from_a.at[turn, rows, :], dir_send.at[2, turn], dir_recv.at[1, turn], dev_a).start()

                    @pl.when((core == k) & (turn >= EARLY))
                    def _():
                        send(src, from_c.at[turn - EARLY, rows, :], dir_send.at[2, turn], dir_recv.at[1, turn], dev_a).start()

                    @pl.when((core == k) & (turn < EARLY))
                    def _():
                        send(src, from_b.at[turn, rows, :], dir_send.at[3, turn], dir_recv.at[2, turn], dev_b).start()

                @pl.when(turn >= EARLY)
                def _():
                    pltpu.make_async_copy(src, from_c.at[turn + 5 - 2 * EARLY, rows, :], dir_send.at[3, turn]).start()

                send(src, pair.at[turn, rows, :], dir_send.at[1, turn], dir_recv.at[0, turn], partner).start()

    def block(turn, carry):
        for k in range(HOPS):
            pos = STRIPS - 1 - LAG + HOPS * (turn - HOP_FROM) + k

            @pl.when((turn >= HOP_FROM) & (pos < STRIPS))
            def _():
                hop(pos, 0)
        idx = slot_at(my_chip, core, turn)
        in_chip = 5 * core + idx
        strip, tall = tile_at(my_chip, in_chip)
        for half in (0, 1):
            source = jnp.where(strip == 9, jnp.where(on_first, 0, 1), half)
            for part in (0, 1):
                rows = pl.ds(0, ROWS_OF[part])

                @pl.when((tall == part) & ((strip < 9) | (half == 0)))
                def _():
                    wait_bytes(first.at[idx, half, rows, :], first_sem.at[idx, half])
                    wait_bytes(second.at[idx, half, rows, :], second_sem.at[idx, half])

                    @pl.when(source != core)
                    def _():
                        wait_bytes(home.at[idx, half, rows, :], home_sem.at[idx])

                    @pl.when(source == core)
                    def _():
                        for grad in (0, 1):
                            @pl.when(on_first == (grad == 0))
                            def _():
                                turn5 = strip % 5 if grad == 0 else (2 * (strip % 5)) % 5
                                pos = 4 * turn5 + 2 * (strip // 5) + grad
                                wait_bytes(home.at[idx, half, rows, :], unit_sem.at[pos * 2 + part])
        for k, src in enumerate((home, first, second)):
            pltpu.make_async_copy(src.at[idx], piece_buf.at[k], piece_sem.at[k]).start()
        for k, src in enumerate((home, first, second)):
            wait_bytes(piece_buf.at[k], piece_sem.at[k])
        n_rows = jnp.where(tall == 0, 512, 384)
        n_cols = jnp.where(strip == 9, 256, 512)
        for half in (0, 1):
            here = pl.ds(half * HALF, HALF)
            value = ((piece_buf[0, half] + piece_buf[1, half]) + piece_buf[2, half]) * scale
            tile_a[:, here] = jnp.where((row[:, :HALF] < n_rows) & (col[:, :HALF] + half * HALF < n_cols), value, 0.0)

        @pl.when(on_first)
        def _():
            tile_b[...] = tile_a[...]

        @pl.when(~on_first)
        def _():
            tile_b[...] = tile_a[...].T

        for k in range(6):
            wait_bytes(state_buf.at[k], state_sem.at[k])
        split(tile_b[...], 0)
        split(state_buf[1], 2)
        nat_rows = jnp.where(on_first, n_rows, n_cols)
        nat_cols = jnp.where(on_first, n_cols, n_rows)

        def rows_step(r, sums):
            here = pl.ds(pl.multiple_of(r * chunk, chunk), chunk)
            pre = times(times(state_buf[0, here, :], 0), 2)
            pre = jnp.where((row[:chunk] + r * chunk < nat_rows) & (col[:chunk] < nat_cols), pre, 0.0)
            tile_a[here, :] = pre
            grad = tile_b[here, :]
            sq_now = STAT_DECAY * state_buf[2, here, :] + (1.0 - STAT_DECAY) * grad * grad
            state_buf[2, here, :] = sq_now
            graft = grad / (jnp.sqrt(sq_now / BIAS_CORR) + GRAFT_EPS)
            return sums[0] + jnp.sum(graft * graft, keepdims=True), sums[1] + jnp.sum(pre * pre, keepdims=True)

        zero = jnp.zeros((1, 1), F32)
        graft_sum, pre_sum = lax.fori_loop(0, BLK // chunk, rows_step, (zero, zero))
        ratio = jnp.sqrt(graft_sum) / jnp.sqrt(pre_sum)
        state_buf[3] = MOM_DECAY * state_buf[3] + tile_a[...] * ratio
        dirs = narrow.at[0, pl.ds(pl.multiple_of(turn * BLK, BLK), BLK), pl.ds(0, BLK)]

        @pl.when(on_first)
        def _():
            dirs[...] = state_buf[3].astype(BF16)

        @pl.when(~on_first)
        def _():
            dirs[...] = state_buf[3].T.astype(BF16)

        @pl.when(turn == SEND_FROM)
        def _():
            for k in range(SEND_FROM):
                leave(k)

        @pl.when(turn >= SEND_FROM)
        def _():
            leave(turn)

        def stats_step(r, carry):
            here = pl.ds(pl.multiple_of(r * chunk, chunk), chunk)
            high = narrow[1, pl.ds(0, BLK), pl.ds(0, BLK)]
            low = narrow[1, pl.ds(BLK, BLK), pl.ds(0, BLK)]
            dot = functools.partial(lax.dot_general, preferred_element_type=F32)
            nt, tn = (((1,), (1,)), ((), ())), (((0,), (0,)), ((), ()))
            a_high = narrow[1, here, pl.ds(0, BLK)]
            a_low = narrow[1, pl.ds(pl.multiple_of(BLK + r * chunk, chunk), chunk), pl.ds(0, BLK)]
            state_buf[4, here, :] = STAT_DECAY * state_buf[4, here, :] + (1.0 - STAT_DECAY) * (
                dot(a_high, high, nt) + (dot(a_high, low, nt) + dot(a_low, high, nt)))
            b_high = narrow[1, pl.ds(0, BLK), here]
            b_low = narrow[1, pl.ds(BLK, BLK), here]
            state_buf[5, here, :] = STAT_DECAY * state_buf[5, here, :] + (1.0 - STAT_DECAY) * (
                dot(b_high, high, tn) + (dot(b_high, low, tn) + dot(b_low, high, tn)))
            return carry

        lax.fori_loop(0, BLK // chunk, stats_step, 0)
        for k, dst in enumerate((new_sq, new_mom, new_left, new_right)):
            pltpu.make_async_copy(state_buf.at[2 + k], dst.at[idx], out_sem.at[k]).start()
        for k in range(4):
            wait_bytes(state_buf.at[2 + k], out_sem.at[k])

        @pl.when(turn < 4)
        def _():
            fetch_state(turn + 1)

        return carry

    lax.fori_loop(0, 5, block, 0)

    def drain(pos, carry):
        @pl.when(kept(pos))
        def _():
            for part in (0, 1):
                u = unit(pos, part)

                @pl.when(~(u['mine'] & (u['own_core'] == core)))
                def _():
                    wait_bytes(u['src'], u['sem'])

        return carry

    lax.fori_loop(0, STRIPS, drain, 0)

    x_chip, y_chip = x_dev // 2, y_dev // 2
    a_chip, b_chip = jnp.where(core == 0, x_chip, y_chip), jnp.where(core == 0, y_chip, x_chip)

    def tall_of(chip, its_core, turn):
        return tile_at(chip, 5 * its_core + slot_at(chip, its_core, turn))[1]

    def hand_on(turn, carry):
        for part in (0, 1):
            rows = pl.ds(0, ROWS_OF[part])
            ref = own.at[turn, rows, :]

            @pl.when(tall_of(a_chip, core, turn) == part)
            def _():
                wait_bytes(ref, dir_recv.at[1, turn])

                @pl.when(turn < EARLY)
                def _():
                    send(from_a.at[turn, rows, :], pair_a.at[turn, rows, :], pass_send.at[0, turn], pass_recv.at[0, turn], partner).start()

                @pl.when(turn >= EARLY)
                def _():
                    send(from_c.at[turn - EARLY, rows, :], pair_a.at[turn, rows, :], pass_send.at[0, turn], pass_recv.at[0, turn], partner).start()

            @pl.when((tall_of(b_chip, core, turn) == part) & (turn < EARLY))
            def _():
                wait_bytes(ref, dir_recv.at[2, turn])
                send(from_b.at[turn, rows, :], pair_b.at[turn, rows, :], pass_send.at[1, turn], pass_recv.at[1, turn], partner).start()
        return carry

    lax.fori_loop(0, 5, hand_on, 0)

    def dirs_done(turn, carry):
        for part in (0, 1):
            ref = own.at[turn, pl.ds(0, ROWS_OF[part]), :]

            @pl.when(tall_of(my_chip, core, turn) == part)
            def _():
                for lane in range(4):
                    wait_bytes(ref, dir_send.at[lane, turn])

            for sem, chip, its_core, turns in ((dir_recv.at[0, turn], my_chip, 1 - core, 5), (pass_send.at[0, turn], a_chip, core, 5),
                                               (pass_send.at[1, turn], b_chip, core, EARLY), (pass_recv.at[0, turn], b_chip, 1 - core, 5),
                                               (pass_recv.at[1, turn], a_chip, 1 - core, EARLY)):
                @pl.when((tall_of(chip, its_core, turn) == part) & (turn < turns))
                def _():
                    wait_bytes(ref, sem)
        return carry

    lax.fori_loop(0, 5, dirs_done, 0)


def step_blocks(n_dev, x_in, dy_mid, x_mid, dy_out, root_left, root_right, graft_sq, momentum, stat_left, stat_right):
    tokens, n_model = x_in.shape
    piece = jax.ShapeDtypeStruct((5, 2, BLK, HALF), F32)
    tile = jax.ShapeDtypeStruct((5, BLK, BLK), F32)
    dirs, early, late = (jax.ShapeDtypeStruct((k, BLK, BLK), BF16) for k in (5, EARLY, 10 - 2 * EARLY))
    dma = pltpu.SemaphoreType.DMA
    outs = pl.pallas_call(
        functools.partial(step_kernel, 1.0 / n_dev),
        out_shape=(piece, piece, piece, tile, tile, tile, tile, dirs, dirs, early, late, early, dirs, early),
        in_specs=[ANY] * 10,
        out_specs=(ANY,) * 14,
        scratch_shapes=[
            pltpu.VMEM((2, tokens, n_model), BF16),
            pltpu.VMEM((3, tokens, HALF), BF16),
            pltpu.VMEM((2, n_model, HALF), F32),
            pltpu.VMEM((STRIPS, n_model, HALF), F32),
            pltpu.VMEM((12, BLK, HALF), F32),
            pltpu.VMEM((3, 2, BLK, HALF), F32),
            pltpu.VMEM((6, BLK, BLK), F32),
            pltpu.VMEM((BLK, BLK), F32),
            pltpu.VMEM((BLK, BLK), F32),
            dma((2,)), dma((3,)), dma((2,)), dma((STRIPS,)), dma((2 * STRIPS,)), dma((12,)), dma((5, 2)), dma((5, 2)), dma((5,)),
            dma((3,)), dma((6,)), dma((4,)), dma((4, 5)), dma((3, 5)), dma((2, 5)), dma((2, 5)),
        ],
        compiler_params=pltpu.CompilerParams(collective_id=0, has_side_effects=True, vmem_limit_bytes=VMEM_MAX),
        name='step_blocks',
    )(x_in, dy_mid, x_mid, dy_out, root_left, root_right, graft_sq, momentum, stat_left, stat_right)
    return outs[3:]


def pass_kernel(*refs):
    for src, dst in zip(refs[:4], refs[4:]):
        dst[...] = src[...]


def pass_on(states):
    spec = pl.BlockSpec((1, BLK, BLK), lambda i: (i, 0, 0))
    return pl.pallas_call(
        pass_kernel,
        grid=(states[0].shape[0],),
        out_shape=tuple(jax.ShapeDtypeStruct(x.shape, x.dtype) for x in states),
        in_specs=[spec] * 4,
        out_specs=(spec,) * 4,
        compiler_params=pltpu.CompilerParams(vmem_limit_bytes=VMEM_MAX),
        cost_estimate=pl.CostEstimate(flops=10 ** 10, bytes_accessed=42 * 10 ** 6, transcendentals=0),
        name='pass_on',
    )(*states)


BUFS, AHEAD = 5, 4


def apply_kernel(places, *refs):
    n_src = 1 + max(place[0] for place in places)
    srcs, (w1, w2) = refs[:n_src], refs[n_src:n_src + 2]
    outs = refs[-8:-6]
    dir_buf, w_buf, o_buf, dir_sem, w_sem, o_sem = refs[-6:]
    me = lax.axis_index('dp')
    core, my_chip = me % 2, me // 2
    x_chip, y_chip, far_chip = flip(me, 2) // 2, flip(me, 4) // 2, flip(me, 6) // 2
    a_chip, b_chip = jnp.where(core == 0, x_chip, y_chip), jnp.where(core == 0, y_chip, x_chip)
    chips = dict(own=my_chip, a=a_chip, b=b_chip, far=far_chip)
    counts = [place[2] for place in places]
    starts = [sum(counts[:k]) for k in range(len(places))]
    n_tiles = sum(counts)

    def tile(n):
        which, spot, turn, chip, its_core = 0, n, n, my_chip, core
        for k, (_, offset, _, name, same, begin) in enumerate(places):
            here = n >= starts[k]
            which = jnp.where(here, k, which)
            spot = jnp.where(here, n - starts[k] + offset, spot)
            turn = jnp.where(here, n - starts[k] + begin, turn)
            chip = jnp.where(here, chips[name], chip)
            its_core = jnp.where(here, core if same else 1 - core, its_core)
        strip, tall = tile_at(chip, 5 * its_core + slot_at(chip, its_core, turn))
        return which, spot, chip, strip, tall

    def window(n, do):
        _, _, chip, strip, tall = tile(n)
        for tall_k in (0, 1):
            for last in (0, 1):
                big, small = ROWS_OF[tall_k], (512, 256)[last]
                at = pl.multiple_of(strip * BLK, BLK)
                here = (tall == tall_k) & ((strip == 9) == (last == 1))

                @pl.when(here & (chip < 2))
                def _():
                    do(0, (pl.ds(tall_k * BLK, big), pl.ds(at, small)), (pl.ds(0, big), pl.ds(0, small)))

                @pl.when(here & (chip >= 2))
                def _():
                    do(1, (pl.ds(at, small), pl.ds(tall_k * BLK, big)), (pl.ds(0, small), pl.ds(0, big)))

    def load(n):
        which, spot, _, _, _ = tile(n)
        slot = n % BUFS
        for k, place in enumerate(places):
            @pl.when(which == k)
            def _():
                pltpu.make_async_copy(srcs[place[0]].at[spot], dir_buf.at[slot], dir_sem.at[slot]).start()
        window(n, lambda k, at, view: pltpu.make_async_copy((w1, w2)[k].at[at], w_buf.at[slot].at[view], w_sem.at[slot]).start())

    def load_wait(n):
        slot = n % BUFS
        wait_bytes(dir_buf.at[slot], dir_sem.at[slot])
        window(n, lambda k, at, view: wait_bytes(w_buf.at[slot].at[view], w_sem.at[slot]))

    def store_wait(n):
        slot = n % BUFS
        window(n, lambda k, at, view: wait_bytes(o_buf.at[slot].at[view], o_sem.at[slot]))

    for n in range(AHEAD):
        load(n)

    def step(n, carry):
        slot = n % BUFS

        @pl.when(n + AHEAD < n_tiles)
        def _():
            load(n + AHEAD)

        load_wait(n)

        @pl.when(n >= BUFS)
        def _():
            store_wait(n - BUFS)

        chip = tile(n)[2]

        @pl.when(chip < 2)
        def _():
            o_buf[slot] = w_buf[slot] - LEARN_RATE * (dir_buf[slot].astype(F32) + WEIGHT_DECAY * w_buf[slot])

        @pl.when(chip >= 2)
        def _():
            o_buf[slot] = w_buf[slot] - LEARN_RATE * (dir_buf[slot].astype(F32).T + WEIGHT_DECAY * w_buf[slot])

        window(n, lambda k, at, view: pltpu.make_async_copy(o_buf.at[slot].at[view], outs[k].at[at], o_sem.at[slot]).start())
        return carry

    lax.fori_loop(0, n_tiles, step, 0)
    for n in range(n_tiles - BUFS, n_tiles):
        store_wait(n)


def apply_update(places, srcs, w1, w2, partial=()):
    dma = pltpu.SemaphoreType.DMA
    n_in = len(srcs) + 2
    share = sum(place[2] for place in places) / 40
    return pl.pallas_call(
        functools.partial(apply_kernel, places),
        out_shape=(jax.ShapeDtypeStruct(w1.shape, F32), jax.ShapeDtypeStruct(w2.shape, F32)),
        in_specs=[ANY] * (n_in + len(partial)),
        out_specs=(ANY, ANY),
        scratch_shapes=[
            pltpu.VMEM((BUFS, BLK, BLK), BF16), pltpu.VMEM((BUFS, BLK, BLK), F32), pltpu.VMEM((BUFS, BLK, BLK), F32),
            dma((BUFS,)), dma((BUFS,)), dma((BUFS,)),
        ],
        input_output_aliases={n_in: 0, n_in + 1: 1} if partial else {},
        compiler_params=pltpu.CompilerParams(vmem_limit_bytes=VMEM_MAX),
        cost_estimate=pl.CostEstimate(flops=int(share * 20 * 10 ** 9), bytes_accessed=int(share * 88 * 10 ** 6), transcendentals=0),
        name='apply_update',
    )(*srcs, w1, w2, *partial)


def solution(mesh):
    n_dev = mesh.shape['dp']
    swap = [(i, i ^ 1) for i in range(n_dev)]
    onward = [(i, i ^ (4 if i % 2 == 0 else 2)) for i in range(n_dev)]

    def per_device(x_in, dy_mid, x_mid, dy_out, w_fc1, w_fc2, stat_left, stat_right, root_left, root_right, graft_sq, momentum):
        *states, own, pair, from_a, from_c, from_b, pair_a, pair_b = step_blocks(
            n_dev, x_in, dy_mid, x_mid, dy_out, root_left, root_right, graft_sq, momentum, stat_left, stat_right)
        far = lax.ppermute(from_a, 'dp', onward)
        far_late = lax.ppermute(from_c, 'dp', onward)
        last = 5 - EARLY
        near = ((0, 0, 5, 'own', True, 0), (1, 0, 5, 'own', False, 0), (2, 0, EARLY, 'a', True, 0), (3, 0, last, 'a', True, EARLY),
                (4, 0, EARLY, 'b', True, 0), (5, 0, 5, 'b', False, 0), (6, 0, EARLY, 'a', False, 0))
        partial = apply_update(near, (own, pair, from_a, from_c, from_b, pair_a, pair_b), w_fc1, w_fc2)
        far, partial, *states = lax.optimization_barrier((far, partial, *states))
        pair_far = lax.ppermute(far, 'dp', swap)
        new_left, new_right, new_sq, new_mom = pass_on(states)
        far_late, new_mom = lax.optimization_barrier((far_late, new_mom))
        pair_far_late = lax.ppermute(far_late, 'dp', swap)
        early = ((0, 0, EARLY, 'far', True, 0), (1, 0, EARLY, 'far', False, 0))
        partial = apply_update(early, (far, pair_far), w_fc1, w_fc2, partial)
        late = ((0, 0, last, 'far', True, EARLY), (0, last, last, 'b', True, EARLY), (1, 0, last, 'far', False, EARLY), (1, last, last, 'a', False, EARLY))
        new_w1, new_w2 = apply_update(late, (far_late, pair_far_late), w_fc1, w_fc2, partial)
        return new_w1, new_w2, new_left, new_right, new_sq, new_mom

    row_spec = P('dp', None)
    rep_spec = P(None, None)
    tile_spec = P('dp', None, None)
    in_specs = (row_spec, row_spec, row_spec, row_spec, rep_spec, rep_spec, tile_spec, tile_spec, tile_spec, tile_spec, tile_spec, tile_spec)
    out_specs = (rep_spec, rep_spec, tile_spec, tile_spec, tile_spec, tile_spec)
    return jax.shard_map(per_device, mesh=mesh, in_specs=in_specs, out_specs=out_specs, check_vma=False)
```
